32 devices in a mesh: frames: 8 (over z, x), heads: 4 (over y, core).
Axes of the slice: x: 2, y: 2, z: 4, core: 2. Of those that a mesh axis runs over, the one named last changes fastest.
Arguments:
- queries: bfloat16 [8192, 2560], P('frames', 'heads'), may hold values from -6 to 6, as said below
- keys: bfloat16 [8192, 2560], P('frames', 'heads'), may hold values from -6 to 6, as said below
- values: bfloat16 [8192, 2560], P('frames', 'heads'), may hold values from -6 to 6
- block_ids: int32 [64, 4], replicated, may hold values from 0 to 63, as said below
- counts: int32 [64], P('frames'), may hold values from 1 to 4
- w_out: bfloat16 [2560, 5120], P('heads'), may hold values from -0.125 to 0.125
Outputs:
- projected: bfloat16 [8192, 5120], P('frames', 'heads')
The draws below stay inside these ranges and needn't reach their ends.
Inputs may be any that keep to these rules, and one draw needn't show every extreme that they name: `block_ids`: block j is held by index j // 8 of frames. Counted with repeats, the entries of the 8 query blocks of one index of frames name at most 4 blocks held by any one index, and exactly 4 held by some index. Entries of a row may repeat. `queries`: drawn in float32 and rounded once. `keys`: drawn in float32 and rounded once.
All inputs are finite; a program needn't handle non-finite values.
Results may differ from the reference program's by a relative error of at most 0.0052.
Values may be sent and summed in bfloat16 or wider, within the bound.
No kernel may reach another device: no remote copies, remote signals or barrier semaphores. Data moves between devices by JAX's collectives and lax.ppermute only.
A program may use at most 192 MiB of HBM per device.

```python
import jax
import jax.numpy as jnp
from jax import lax

D = 5120
HEADS = 20
DH = 128
TILE = 128
SEL = 4
BLK_DEV = 8
NB = 64
TOKENS = 8192
CAP = 4
N_FRAMES = 8


def pair_draw(key, which_one):
    base = jax.random.fold_in(key, 7)
    key_query, key_key = jax.random.split(base, 2)
    full_shape = (TOKENS, HEADS * DH)
    query_part = jnp.clip(1.5 * jax.random.normal(key_query, full_shape, jnp.float32), -6.0, 6.0)
    key_part = jnp.clip(1.5 * jax.random.normal(key_key, full_shape, jnp.float32), -6.0, 6.0)
    if which_one == 0:
        return query_part
    return key_part


def draw_queries(key, part):
    return pair_draw(key, 0).astype(jnp.bfloat16)


def draw_keys(key, part):
    return pair_draw(key, 1).astype(jnp.bfloat16)


def draw_block_ids(key, part):
    requests = BLK_DEV * SEL

    def one_device(device_key):
        key_star, key_order, key_shuffle, key_local = jax.random.split(device_key, 4)
        owners = jnp.tile(jnp.arange(N_FRAMES, dtype=jnp.int32), CAP)
        star = jax.random.randint(key_star, (), 0, N_FRAMES, dtype=jnp.int32)
        order = jax.random.permutation(key_order, N_FRAMES * CAP).astype(jnp.int32)
        priority = order + jnp.where(owners == star, 0, N_FRAMES * CAP).astype(jnp.int32)
        picked = owners[jnp.argsort(priority, stable=True)][:requests]
        shuffled = picked[jax.random.permutation(key_shuffle, requests)]
        local_block = jax.random.randint(key_local, (requests,), 0, BLK_DEV, dtype=jnp.int32)
        return shuffled * BLK_DEV + local_block
    device_keys = jax.vmap(lambda device: jax.random.fold_in(key, 100 + device))(jnp.arange(N_FRAMES))
    return jax.vmap(one_device)(device_keys).reshape(NB, SEL).astype(jnp.int32)


def place_ends(array, key, least, top_value):
    spot = [jax.random.randint(jax.random.fold_in(key, axis), (), 0, length) for axis, length in enumerate(array.shape)]
    main_axis = array.shape.index(max(array.shape))
    beside = spot[:main_axis] + [(spot[main_axis] + 1) % array.shape[main_axis]] + spot[main_axis + 1:]
    return array.at[tuple(spot)].set(least).at[tuple(beside)].set(top_value)


def level_of(own_key, shape, cuts, least, top_value):
    def one(axis_at, shards_of):
        draws = jax.random.uniform(jax.random.fold_in(jax.random.fold_in(own_key, 6), axis_at), (shards_of,), jnp.float32, least / len(cuts), top_value / len(cuts))
        return jnp.repeat(jnp.exp(draws), shape[axis_at] // shards_of).reshape((-1,) + (1,) * (len(shape) - axis_at - 1))

    loudness = one(*cuts[0])
    for cut in cuts[1:]:
        loudness = loudness * one(*cut)
    return loudness


def normal_values(key, extent, scale, reach, cuts=(), kind=jnp.bfloat16):
    loudness = level_of(key, extent, cuts, -0.22, 0.18) if cuts else 1.0
    array = jax.random.normal(key, extent, jnp.float32) * scale * loudness
    return jnp.minimum(jnp.maximum(array, -reach), reach).astype(kind)


def setup_inputs(seed: int = 0) -> dict:
    arg_keys = jax.random.split(jax.random.key(seed), 7)
    queries = draw_queries(jax.random.fold_in(arg_keys[6], 71), 0)
    keys = draw_keys(jax.random.fold_in(arg_keys[6], 71), 0)
    values = normal_values(arg_keys[2], (TOKENS, HEADS * DH), 1.0, 6.0, ((0, 8), (1, 4)))
    block_ids = draw_block_ids(jax.random.fold_in(arg_keys[6], 71), 0)
    counts = place_ends(jax.random.randint(arg_keys[4], (NB,), 1, SEL + 1), jax.random.fold_in(arg_keys[4], 1), 1, SEL).astype(jnp.int32)
    w_out = normal_values(arg_keys[5], (HEADS * DH, D), (HEADS * DH) ** -0.5, 0.125, ((0, 4),))
    return {"queries": queries, "keys": keys, "values": values, "block_ids": block_ids, "counts": counts, "w_out": w_out}


def reference(queries, keys, values, block_ids, counts, w_out):
    full_width = HEADS * DH
    inv_root = 1.0 / (DH ** 0.5)
    query_tiles = queries.reshape(NB, TILE, full_width)
    key_tiles = keys.reshape(NB, TILE, full_width)
    value_tiles = values.reshape(NB, TILE, full_width)

    def one_block(block_index):
        chosen = block_ids[block_index]
        keyset_k = jnp.concatenate([key_tiles[block_index][None], key_tiles[chosen]], 0)
        keyset_v = jnp.concatenate([value_tiles[block_index][None], value_tiles[chosen]], 0)
        keyset_k = keyset_k.reshape((SEL + 1) * TILE, HEADS, DH).astype(jnp.float32)
        keyset_v = keyset_v.reshape((SEL + 1) * TILE, HEADS, DH).astype(jnp.float32)
        query_tile = query_tiles[block_index].reshape(TILE, HEADS, DH).astype(jnp.float32)
        scores = jnp.einsum("qhd,khd->hqk", query_tile, keyset_k) * inv_root
        allowed = jnp.concatenate([jnp.ones((1,), bool), jnp.arange(SEL) < counts[block_index]])
        key_allowed = jnp.repeat(allowed, TILE)
        scores = jnp.where(key_allowed[None, None, :], scores, -jnp.inf)
        row_max = jnp.max(scores, axis=-1, keepdims=True)
        probs = jnp.exp(scores - row_max)
        denom_sum = jnp.sum(probs, axis=-1)
        weights = lax.optimization_barrier(probs.astype(jnp.bfloat16)).astype(jnp.float32)
        mixed = jnp.einsum("hqk,khd->qhd", weights, keyset_v)
        mixed = mixed / jnp.transpose(denom_sum)[:, :, None]
        return mixed.astype(jnp.bfloat16).reshape(TILE, full_width)

    attn = lax.map(one_block, jnp.arange(NB)).reshape(TOKENS, full_width)
    return jnp.dot(attn, w_out, preferred_element_type=jnp.float32).astype(jnp.bfloat16)
```

```python
import functools

import jax
import jax.numpy as jnp
from jax import lax
from jax.experimental import pallas as pl
from jax.experimental.pallas import tpu as pltpu
from jax.sharding import PartitionSpec as P

DH = 128
TILE = 128


def pack_body(index_ref, k_ref, v_ref, *out_refs):
    capacity = out_refs[0].shape[1]
    for i, out_ref in enumerate(out_refs):
        for r in range(capacity):
            start = pl.multiple_of(index_ref[i * capacity + r] * TILE, TILE)
            out_ref[0, r] = k_ref[pl.ds(start, TILE), :]
            out_ref[1, r] = v_ref[pl.ds(start, TILE), :]


def pack(index, keys, values, col, wide, peers, capacity):
    tokens = keys.shape[0]
    kind = jax.ShapeDtypeStruct((2, capacity, TILE, wide), keys.dtype)
    cols = pl.BlockSpec((tokens, wide), lambda i, _: (0, col // wide))
    return pl.pallas_call(
        pack_body,
        out_shape=[kind] * peers,
        grid_spec=pltpu.PrefetchScalarGridSpec(
            num_scalar_prefetch=1,
            grid=(1,),
            in_specs=[cols, cols],
            out_specs=[pl.BlockSpec(kind.shape, lambda i, _: (0, 0, 0, 0))] * peers,
        ),
        cost_estimate=pl.CostEstimate(
            flops=4_000_000, bytes_accessed=4 * tokens * wide * 4, transcendentals=0
        ),
    )(index, keys, values)


def attend_body(slot_ref, count_ref, q_ref, k_ref, v_ref, *refs, select):
    got_refs, (out_ref, pool_k, pool_v) = refs[:-3], refs[-3:]
    tokens, wide = q_ref.shape
    blocks = tokens // TILE
    capacity = got_refs[0].shape[1]
    inv_root = 1.0 / DH**0.5
    for b in range(blocks):
        pool_k[b] = k_ref[b * TILE : (b + 1) * TILE, :]
        pool_v[b] = v_ref[b * TILE : (b + 1) * TILE, :]
    for i, got_ref in enumerate(got_refs):
        for r in range(capacity):
            pool_k[blocks + i * capacity + r] = got_ref[0, r]
            pool_v[blocks + i * capacity + r] = got_ref[1, r]

    def one_block(b, carry):
        rows = pl.ds(pl.multiple_of(b * TILE, TILE), TILE)
        slots = [b] + [slot_ref[b * select + s] for s in range(select)]
        limit = (count_ref[b] + 1) * TILE
        for h in range(wide // DH):
            at = slice(h * DH, (h + 1) * DH)
            kset = jnp.concatenate([pool_k[s, :, at] for s in slots], 0)
            vset = jnp.concatenate([pool_v[s, :, at] for s in slots], 0)
            scores = (
                lax.dot_general(
                    q_ref[rows, at],
                    kset,
                    (((1,), (1,)), ((), ())),
                    preferred_element_type=jnp.float32,
                )
                * inv_root
            )
            place = lax.broadcasted_iota(jnp.int32, scores.shape, 1)
            scores = jnp.where(place < limit, scores, -jnp.inf)
            probs = jnp.exp(scores - jnp.max(scores, axis=-1, keepdims=True))
            denom = jnp.sum(probs, axis=-1, keepdims=True)
            mixed = jnp.dot(
                probs.astype(jnp.bfloat16), vset, preferred_element_type=jnp.float32
            )
            out_ref[rows, at] = (mixed / denom).astype(out_ref.dtype)
        return carry

    lax.fori_loop(0, blocks, one_block, 0)


def attend(slots, counts, queries, keys, values, got, col, wide, select):
    tokens = queries.shape[0]
    pool = tokens // TILE + len(got) * got[0].shape[1]
    cols = pl.BlockSpec((tokens, wide), lambda i, *_: (0, col // wide))
    return pl.pallas_call(
        functools.partial(attend_body, select=select),
        out_shape=jax.ShapeDtypeStruct((tokens, wide), queries.dtype),
        grid_spec=pltpu.PrefetchScalarGridSpec(
            num_scalar_prefetch=2,
            grid=(1,),
            in_specs=[cols, cols, cols]
            + [pl.BlockSpec(got[0].shape, lambda i, *_: (0, 0, 0, 0))] * len(got),
            out_specs=pl.BlockSpec((tokens, wide), lambda i, *_: (0, 0)),
            scratch_shapes=[
                pltpu.VMEM((pool, TILE, wide), keys.dtype),
                pltpu.VMEM((pool, TILE, wide), keys.dtype),
            ],
        ),
        cost_estimate=pl.CostEstimate(
            flops=4 * tokens * wide * (select + 1) * TILE * 4,
            bytes_accessed=tokens * wide * 20,
            transcendentals=tokens * (wide // DH) * (select + 1) * TILE,
        ),
    )(slots, counts, queries, keys, values, *got)


def project_body(*refs, peers, more):
    rows, mats, rest = refs[:peers], refs[peers : 2 * peers], refs[2 * peers :]
    total = rest[0][...] if more else None
    for row_ref, mat_ref in zip(rows, mats):
        part = jnp.dot(row_ref[...], mat_ref[...], preferred_element_type=jnp.float32)
        total = part if total is None else total + part
    rest[-1][...] = total.astype(rest[-1].dtype)


def project(rows, mats, total, col, wide, kind):
    tokens = rows[0].shape[0]
    width = mats[0].shape[1]
    step = 256
    more = total is not None
    out_spec = pl.BlockSpec((tokens, step), lambda j: (0, j))
    return pl.pallas_call(
        functools.partial(project_body, peers=len(rows), more=more),
        out_shape=jax.ShapeDtypeStruct((tokens, width), kind),
        grid=(width // step,),
        in_specs=[pl.BlockSpec((tokens, wide), lambda j: (0, 0))] * len(rows)
        + [pl.BlockSpec((wide, step), lambda j: (col // wide, j))] * len(rows)
        + [out_spec] * more,
        out_specs=out_spec,
        cost_estimate=pl.CostEstimate(
            flops=2 * tokens * wide * width * len(rows),
            bytes_accessed=tokens * width * 8,
            transcendentals=0,
        ),
    )(*rows, *mats, *([total] if more else []))


def swap(array, axis, mask):
    size = lax.axis_size(axis)
    return lax.ppermute(array, axis, [(i, i ^ mask) for i in range(size)])


def shards(queries, keys, values, block_ids, counts, w_out):
    frame_count = lax.axis_size("frames")
    here = lax.axis_index("frames")
    head_count = lax.axis_size("heads")
    head_here = lax.axis_index("heads")
    tokens_here, width = queries.shape
    blocks = tokens_here // TILE
    select = block_ids.shape[1]
    requests = blocks * select
    capacity = max(2, (requests + frame_count - 1) // frame_count)

    masks = sorted(range(1, frame_count), reverse=True)
    mask_list = jnp.array(masks, jnp.int32)
    wanted = block_ids.reshape(frame_count, requests)
    is_mine = (wanted // blocks) == here
    mine_count = is_mine.astype(jnp.int32)
    rank = jnp.cumsum(mine_count, axis=1) - mine_count
    hit = is_mine[:, :, None] & (
        rank[:, :, None] == jnp.arange(capacity, dtype=jnp.int32)[None, None, :]
    )
    send_index = jnp.sum(jnp.where(hit, (wanted % blocks)[:, :, None], 0), axis=1)
    peers = here ^ mask_list
    send_index = jnp.sum(
        jnp.where(
            peers[:, None, None] == jnp.arange(frame_count, dtype=jnp.int32)[None, :, None],
            send_index[None],
            0,
        ),
        axis=1,
    ).reshape(-1)

    mine = lax.dynamic_slice_in_dim(wanted, here, 1, 0).reshape(requests)
    owner = mine // blocks
    order = jnp.arange(requests, dtype=jnp.int32)
    earlier = (owner[None, :] == owner[:, None]) & (order[None, :] < order[:, None])
    my_rank = jnp.sum(earlier.astype(jnp.int32), axis=1)
    place = (frame_count - 1) - (owner ^ here)
    slots = jnp.where(owner == here, mine % blocks, blocks + place * capacity + my_rank)

    chunks = []
    at = 0
    while at < width:
        wide = 2 * DH if at + 2 * DH <= width else DH
        chunks.append((at, wide))
        at += wide

    got = []
    for at, wide in chunks:
        packed = pack(send_index, keys, values, at, wide, len(masks), capacity)
        got.append([swap(part, "frames", m) for part, m in zip(packed, masks)])
        if at == 0:
            out_width = w_out.shape[1] // head_count
            mats = []
            for m in range(head_count):
                part = lax.dynamic_slice_in_dim(
                    w_out, (head_here ^ m) * out_width, out_width, 1
                )
                mats.append(swap(part, "heads", m) if m else part)

    total = None
    for i, (at, wide) in enumerate(chunks):
        rows = [attend(slots, counts, queries, keys, values, got[i], at, wide, select)]
        tags = [0]
        m = head_count // 2
        while m:
            rows = rows + [swap(r, "heads", m) for r in rows]
            tags = tags + [t ^ m for t in tags]
            m //= 2
        last = i == len(chunks) - 1
        total = project(
            rows,
            [mats[t] for t in tags],
            total,
            at,
            wide,
            jnp.bfloat16 if last else jnp.float32,
        )
    return total


def solution(mesh):
    placed = (
        P("frames", "heads"),
        P("frames", "heads"),
        P("frames", "heads"),
        P(),
        P("frames"),
        P("heads", None),
    )
    return jax.shard_map(
        shards, mesh=mesh, in_specs=placed, out_specs=P("frames", "heads"), check_vma=False
    )
```
